32 devices in a mesh: grp: 4 (over y, x), row: 8 (over z, core).
Axes of the slice: x: 2, y: 2, z: 4, core: 2. Of those that a mesh axis runs over, the one named last changes fastest.
Arguments:
- a_tiles: bfloat16 [64, 4, 7, 128, 128], P('row', 'grp'), may hold values from -0.5 to 0.5
- a_cols: int32 [64, 4, 7], P('row', 'grp'), may hold values from 0 to 63, as said below
- p_tiles: bfloat16 [64, 4, 128, 128], P('row'), may hold values from -0.5 to 0.5
- p_cols: int32 [64, 4], replicated, may hold values from 0 to 31, as said below
- c_cols: int32 [32, 16], replicated, may hold values from 0 to 31, as said below
Outputs:
- coarse: float32 [32, 16, 128, 128], P('row', 'grp')
The draws below stay inside these ranges and needn't reach their ends.
Inputs may be any that keep to these rules, and one draw needn't show every extreme that they name: For fine tile row i in block b = i // 8, every entry of a_cols[i] lies in [max(b - 2, 0) * 8, min(b + 3, 8) * 8). For fine tile row i in block b = i // 8, the entries of p_cols[i] are distinct and lie in [(b - 1) * 4, (b + 2) * 4). For coarse tile row c in block t = c // 4, the entries of c_cols[c] are distinct and lie among the 20 coarse tile rows that start at min(max(t - 2, 0), 3) * 4.
All inputs are finite; a program needn't handle non-finite values.
Results may differ from the reference program's by a relative error of at most 0.0003.
Values may be sent and summed in bfloat16 or wider, within the bound.
A program may use at most 128 MiB of HBM per device.

```python
import jax
import jax.numpy as jnp
from jax import lax

TILE = 128
CT_DEV = 4
SLOTS = 7
KP = 4
KC = 16
FT_DEV = 8
GROUPS = 4
FT = 64
NCT = 32


def pick_distinct(key, count, width, valid, take):
    offsets = jnp.arange(width, dtype=jnp.int32)[None, :]
    scores = jax.random.randint(key, (count, width), 0, 1 << 20, dtype=jnp.int32) * width + offsets
    scores = jnp.where(valid, scores, -1 - offsets)
    top_scores, chosen = lax.top_k(scores, take)
    return chosen.astype(jnp.int32)


def draw_a_cols(key, part):
    fine_ids = jnp.arange(FT, dtype=jnp.int32)
    owner = fine_ids // FT_DEV
    lowest = jnp.maximum(owner - 2, 0) * FT_DEV
    highest_row = jnp.minimum(owner + 3, FT // FT_DEV) * FT_DEV
    spans = (highest_row - lowest)[:, None, None]
    picks = jax.random.randint(jax.random.fold_in(key, 17), (FT, GROUPS, SLOTS), 0, 1 << 30, dtype=jnp.int32)
    return (lowest[:, None, None] + picks % spans).astype(jnp.int32)


def draw_p_cols(key, part):
    fine_ids = jnp.arange(FT, dtype=jnp.int32)
    owner = fine_ids // FT_DEV
    begin = (owner - 1) * CT_DEV
    candidate = begin[:, None] + jnp.arange(3 * CT_DEV, dtype=jnp.int32)[None, :]
    valid = (candidate >= 0) & (candidate < NCT)
    chosen = pick_distinct(jax.random.fold_in(key, 29), FT, 3 * CT_DEV, valid, KP)
    return (begin[:, None] + chosen).astype(jnp.int32)


def draw_c_cols(key, part):
    coarse_ids = jnp.arange(NCT, dtype=jnp.int32)
    owner = coarse_ids // CT_DEV
    begin = jnp.clip(owner - 2, 0, NCT // CT_DEV - 5) * CT_DEV
    valid = jnp.ones((NCT, 5 * CT_DEV), dtype=bool)
    chosen = pick_distinct(jax.random.fold_in(key, 41), NCT, 5 * CT_DEV, valid, KC)
    return (begin[:, None] + chosen).astype(jnp.int32)


def block_levels(own_key, dims, pieces, least, high):
    gain = 1.0
    for axis_at, blocks in pieces:
        draws = jax.random.uniform(jax.random.fold_in(jax.random.fold_in(own_key, 6), axis_at), (blocks,), jnp.float32, least / len(pieces), high / len(pieces))
        gain = gain * jnp.repeat(jnp.exp(draws), dims[axis_at] // blocks).reshape((-1,) + (1,) * (len(dims) - 1 - axis_at))
    return gain


def normal_values(rng, dims, scale, bound, split=(), kind=jnp.bfloat16):
    loudness = block_levels(rng, dims, split, -0.22, 0.18) if split else 1.0
    entries = jax.random.normal(rng, dims, jnp.float32) * scale * loudness
    return jnp.minimum(jnp.maximum(entries, -bound), bound).astype(kind)


def setup_inputs(seed: int = 0) -> dict:
    splits = jax.random.split(jax.random.key(seed), 6)
    a_tiles = normal_values(splits[0], (FT, GROUPS, SLOTS, TILE, TILE), TILE ** -0.5, 0.5, ((0, 8), (1, 4)))
    a_cols = draw_a_cols(jax.random.fold_in(splits[5], 71), 0)
    p_tiles = normal_values(splits[2], (FT, KP, TILE, TILE), TILE ** -0.5, 0.5, ((0, 8),))
    p_cols = draw_p_cols(jax.random.fold_in(splits[5], 71), 0)
    c_cols = draw_c_cols(jax.random.fold_in(splits[5], 71), 0)
    return dict(a_tiles=a_tiles, a_cols=a_cols, p_tiles=p_tiles, p_cols=p_cols, c_cols=c_cols)


highest = lax.Precision.HIGHEST


def reference(a_tiles, a_cols, p_tiles, p_cols, c_cols):
    def fine_row(coarse, inputs):
        a_row, columns, own_tiles, own_cols = inputs
        targets = c_cols[own_cols]
        fetched = p_tiles[columns].astype(jnp.float32)
        fetched_cols = p_cols[columns]
        products = jnp.einsum("gsxy,gspyz->gspxz", a_row.astype(jnp.float32), fetched, precision=highest)
        matches = (fetched_cols[:, :, :, None, None] == targets[None, None, None, :, :]).astype(jnp.float32)
        partial_value = jnp.einsum("gspxz,gspqk->gqkxz", products, matches, precision=highest)
        summed = jnp.sum(partial_value, axis=0)
        row_terms = jnp.einsum("qyx,qkyz->qkxz", own_tiles.astype(jnp.float32), summed, precision=highest)
        return coarse.at[own_cols].add(row_terms), None

    initial = jnp.zeros((NCT, KC, TILE, TILE), jnp.float32)
    result = lax.scan(fine_row, initial, (a_tiles, a_cols, p_tiles, p_cols))[0]
    return result
```

```python
import functools

import jax
import jax.numpy as jnp
from jax import lax
from jax.experimental import pallas as pl
from jax.experimental.pallas import tpu as pltpu
from jax.sharding import PartitionSpec as P

RATIO = 2
REACH = 2


LEVELS = 32767.0


def encoded(value):
    most = jnp.maximum(jnp.max(jnp.abs(value), axis=0, keepdims=True), 2e-34)
    code = jnp.round(value * (LEVELS / most)).astype(jnp.int32).astype(jnp.int16)
    return code, most * (1.0 / LEVELS)


def decoded(code, scale):
    return code.astype(jnp.int32).astype(jnp.float32) * scale


def product_kernel(
    sizes,
    where,
    a_cols,
    p_cols,
    c_cols,
    a_ref,
    band_ref,
    center_ref,
    codes_ref,
    scales_ref,
    total_ref,
    spread,
    halves,
):
    fine_rows, slots, kp, kc, tile, chunks = sizes
    coarse_rows = fine_rows // RATIO
    window = (2 * (REACH + 1) + 1) * coarse_rows
    position = where[0]
    first_row = position * fine_rows
    band_start = first_row - REACH * fine_rows
    window_start = (position - REACH - 1) * coarse_rows
    base_coarse = (position - 1) * coarse_rows
    total_ref[...] = jnp.zeros_like(total_ref)
    halves[window] = jnp.zeros((2 * tile, tile), jnp.bfloat16)
    group = min(4, kc)

    @pl.loop(0, fine_rows)
    def _(i):
        spread[...] = jnp.zeros_like(spread)
        for s in range(slots):
            j = a_cols[s, 0, i]
            local = (j - band_start) * kp
            right = jnp.concatenate([band_ref[local + p] for p in range(kp)], axis=1)
            prod = jnp.dot(a_ref[i * slots + s], right, preferred_element_type=jnp.float32)
            for p in range(kp):
                w = p_cols[p, j] - window_start
                spread[w] = spread[w] + prod[:, p * tile : (p + 1) * tile]

        @pl.loop(0, window, unroll=4)
        def _(w):
            value = spread[w]
            high = value.astype(jnp.bfloat16)
            halves[w, :tile] = high
            halves[w, tile:] = (value - high.astype(jnp.float32)).astype(jnp.bfloat16)

        for q in range(kp):
            c = p_cols[q, first_row + i]
            own = band_ref[(REACH * fine_rows + i) * kp + q].T
            left = jnp.concatenate([own, own], axis=1)
            out = (c - base_coarse) * kc
            for k in range(0, kc, group):
                parts = []
                for n in range(group):
                    w = c_cols[k + n, c] - window_start
                    w = jnp.where((w < 0) | (w >= window), window, w)
                    parts.append(halves[w])
                prod = jnp.dot(
                    left, jnp.concatenate(parts, axis=1), preferred_element_type=jnp.float32
                )
                for n in range(group):
                    at = out + k + n
                    total_ref[at] = total_ref[at] + prod[:, n * tile : (n + 1) * tile]

    share = kc // chunks
    for chunk in range(chunks):

        @pl.loop(0, coarse_rows)
        def _(c):
            for n in range(share):
                e = c * share + n
                k = chunk * share + n
                center_ref[chunk, e] = total_ref[(coarse_rows + c) * kc + k]
                for side in range(2):
                    value = total_ref[(2 * side * coarse_rows + c) * kc + k]
                    code, scale = encoded(value)
                    codes_ref[side, chunk, e] = code
                    scales_ref[side, chunk, pl.ds(e, 1)] = scale


def local_products(a_tiles, a_cols, band, p_cols, c_cols, position, chunks):
    fine_rows, _, slots, tile, _ = a_tiles.shape
    kp = band.shape[1]
    kc = c_cols.shape[1]
    coarse_rows = fine_rows // RATIO
    window = (2 * (REACH + 1) + 1) * coarse_rows
    members = coarse_rows * kc // chunks
    smem = pl.BlockSpec(memory_space=pltpu.SMEM)
    vmem = pl.BlockSpec(memory_space=pltpu.VMEM)
    return pl.pallas_call(
        functools.partial(product_kernel, (fine_rows, slots, kp, kc, tile, chunks)),
        out_shape=[
            jax.ShapeDtypeStruct((chunks, members, tile, tile), jnp.float32),
            jax.ShapeDtypeStruct((2, chunks, members, tile, tile), jnp.int16),
            jax.ShapeDtypeStruct((2, chunks, members, tile), jnp.float32),
        ],
        in_specs=[smem] * 4 + [vmem] * 2,
        out_specs=[vmem] * 3,
        scratch_shapes=[
            pltpu.VMEM((3 * coarse_rows * kc, tile, tile), jnp.float32),
            pltpu.VMEM((window, tile, tile), jnp.float32),
            pltpu.VMEM((window + 1, 2 * tile, tile), jnp.bfloat16),
        ],
        compiler_params=pltpu.CompilerParams(vmem_limit_bytes=34 * 1024 * 1024),
    )(
        position.reshape(1),
        a_cols.T,
        p_cols.T,
        c_cols.T,
        a_tiles.reshape(-1, tile, tile),
        band.reshape(-1, tile, tile),
    )


def exchange_kernel(
    rows,
    chunks,
    center,
    codes,
    scales,
    out,
    side_codes,
    side_scales,
    sent_codes,
    sent_scales,
    peer_codes,
    peer_scales,
    side_sems,
    side_scale_sems,
    peer_sems,
    peer_scale_sems,
):
    r = lax.axis_index("row")
    g = lax.axis_index("grp")
    members = out.shape[0]
    barrier = pltpu.get_barrier_semaphore()
    mesh_type = pl.DeviceIdType.MESH

    def signal(where):
        pl.semaphore_signal(barrier, inc=1, device_id=where, device_id_type=mesh_type)

    for t in range(chunks - 1):
        signal({"grp": lax.rem(g + 1 + t, chunks)})

    @pl.when(r > 0)
    def _():
        signal({"row": r - 1})

    @pl.when(r < rows - 1)
    def _():
        signal({"row": r + 1})

    inside = (r > 0) & (r < rows - 1)

    @pl.when(inside)
    def _():
        pl.semaphore_wait(barrier, chunks + 1)

    @pl.when(jnp.logical_not(inside))
    def _():
        pl.semaphore_wait(barrier, chunks)

    sends = ((r > 0, r - 1), (r < rows - 1, r + 1))
    comes = (r < rows - 1, r > 0)

    def scale_copy(side):
        return pltpu.make_async_remote_copy(
            src_ref=scales.at[side],
            dst_ref=side_scales.at[side],
            send_sem=side_scale_sems.at[0, side],
            recv_sem=side_scale_sems.at[1, side],
            device_id={"row": sends[side][1]},
            device_id_type=mesh_type,
        )

    def side_copy(side, t):
        return pltpu.make_async_remote_copy(
            src_ref=codes.at[side, lax.rem(g + 1 + t, chunks)],
            dst_ref=side_codes.at[side, t],
            send_sem=side_sems.at[0, side, t],
            recv_sem=side_sems.at[1, side, t],
            device_id={"row": sends[side][1]},
            device_id_type=mesh_type,
        )

    def peer_copy(t):
        return pltpu.make_async_remote_copy(
            src_ref=sent_codes.at[t],
            dst_ref=peer_codes.at[t],
            send_sem=peer_sems.at[0, t],
            recv_sem=peer_sems.at[1, t],
            device_id={"grp": lax.rem(g + 1 + t, chunks)},
            device_id_type=mesh_type,
        )

    def peer_scale_copy(t):
        return pltpu.make_async_remote_copy(
            src_ref=sent_scales.at[t],
            dst_ref=peer_scales.at[t],
            send_sem=peer_scale_sems.at[0, t],
            recv_sem=peer_scale_sems.at[1, t],
            device_id={"grp": lax.rem(g + 1 + t, chunks)},
            device_id_type=mesh_type,
        )

    for side in range(2):

        @pl.when(sends[side][0])
        def _():
            scale_copy(side).start()
            for t in range(chunks):
                side_copy(side, t).start()

        @pl.when(jnp.logical_not(comes[side]))
        def _():
            side_scales[side] = jnp.zeros_like(side_scales[side])

            @pl.loop(0, chunks)
            def _(t):
                @pl.loop(0, members)
                def _(e):
                    side_codes[side, t, e] = jnp.zeros(side_codes.shape[3:], jnp.int16)

    for side in range(2):

        @pl.when(comes[side])
        def _():
            scale_copy(side).wait_recv()

    for t in range(chunks):
        d = lax.rem(g + 1 + t, chunks)
        for side in range(2):

            @pl.when(comes[side])
            def _():
                side_copy(side, t).wait_recv()

        @pl.loop(0, members)
        def _(e):
            value = center[d, e]
            for side in range(2):
                value += decoded(side_codes[side, t, e], side_scales[side, d, pl.ds(e, 1)])
            if t < chunks - 1:
                code, scale = encoded(value)
                sent_codes[t, e] = code
                sent_scales[t, pl.ds(e, 1)] = scale
            else:
                out[e] = value

        if t < chunks - 1:
            peer_scale_copy(t).start()
            peer_copy(t).start()

    for t in range(chunks - 1):
        peer_scale_copy(t).wait_recv()
        peer_copy(t).wait_recv()

        @pl.loop(0, members)
        def _(e):
            out[e] = out[e] + decoded(peer_codes[t, e], peer_scales[t, pl.ds(e, 1)])

    for t in range(chunks - 1):
        peer_scale_copy(t).wait_send()
        peer_copy(t).wait_send()
    for side in range(2):

        @pl.when(sends[side][0])
        def _():
            scale_copy(side).wait_send()
            for t in range(chunks):
                side_copy(side, t).wait_send()


def exchange(center, codes, scales, rows):
    chunks, members, tile, _ = center.shape
    vmem = pl.BlockSpec(memory_space=pltpu.VMEM)
    anywhere = pl.BlockSpec(memory_space=pl.ANY)
    dma = pltpu.SemaphoreType.DMA
    return pl.pallas_call(
        functools.partial(exchange_kernel, rows, chunks),
        out_shape=jax.ShapeDtypeStruct((members, tile, tile), jnp.float32),
        in_specs=[vmem, anywhere, vmem],
        out_specs=vmem,
        scratch_shapes=[
            pltpu.VMEM((2, chunks, members, tile, tile), jnp.int16),
            pltpu.VMEM((2, chunks, members, tile), jnp.float32),
            pltpu.VMEM((chunks - 1, members, tile, tile), jnp.int16),
            pltpu.VMEM((chunks - 1, members, tile), jnp.float32),
            pltpu.VMEM((chunks - 1, members, tile, tile), jnp.int16),
            pltpu.VMEM((chunks - 1, members, tile), jnp.float32),
            dma((2, 2, chunks)),
            dma((2, 2)),
            dma((2, chunks - 1)),
            dma((2, chunks - 1)),
        ],
        compiler_params=pltpu.CompilerParams(
            collective_id=0, has_side_effects=True, vmem_limit_bytes=40 * 1024 * 1024
        ),
    )(center, codes, scales)


def gather_kernel(
    rows,
    groups,
    own,
    band,
    side_sems,
    near_sems,
    pair_sems,
    pass_sems,
    own_sem,
):
    r = lax.axis_index("row")
    g = lax.axis_index("grp")
    odd = lax.rem(r, 2)
    partner = r + 1 - 2 * odd
    has = (r >= 2, r < rows - 2)
    takes = (r < rows - 2, r >= 2)
    blocks = (4, 0)
    targets = (r - 2, r + 2)
    g_odd = lax.rem(g, 2)
    g_high = lax.rem(g // 2, 2)
    near = (g + 1 - 2 * g_odd, g + 2 - 4 * g_high)
    half = own.shape[0] // 2
    parity = lax.rem(g_odd + g_high, 2)
    mine = parity * half
    other = (1 - parity) * half
    barrier = pltpu.get_barrier_semaphore()
    mesh_type = pl.DeviceIdType.MESH
    turn = half // 2
    order = [n * turn + c for c in range(turn) for n in range(2)]

    def copy(src, dst, send, recv, to):
        return pltpu.make_async_remote_copy(
            src_ref=src,
            dst_ref=dst,
            send_sem=send,
            recv_sem=recv,
            device_id=to,
            device_id_type=mesh_type,
        )

    def side(d, c):
        at = mine + c
        return copy(
            own.at[at],
            band.at[blocks[d], at],
            side_sems.at[0, d, c],
            side_sems.at[1, d, c],
            {"row": targets[d]},
        )

    def near_out(d, c):
        at = mine + c
        return copy(
            band.at[blocks[d], at],
            band.at[blocks[d], at],
            near_sems.at[0, d, c],
            near_sems.at[1, d, c],
            {"grp": near[c // turn]},
        )

    def near_in(d, c):
        at = other + c
        return copy(
            band.at[blocks[d], at],
            band.at[blocks[d], at],
            near_sems.at[0, d, c],
            near_sems.at[1, d, c],
            {"grp": near[c // turn]},
        )

    def pair():
        return copy(
            own, band.at[1 + 2 * odd], pair_sems.at[0], pair_sems.at[1], {"row": partner}
        )

    def passed(at):
        return copy(
            band.at[4 - 4 * odd, at],
            band.at[3 - 2 * odd, at],
            pass_sems.at[0, at],
            pass_sems.at[1, at],
            {"row": partner},
        )

    def signal(to):
        pl.semaphore_signal(barrier, inc=1, device_id=to, device_id_type=mesh_type)

    signal({"row": partner})
    signal({"grp": near[0]})
    signal({"grp": near[1]})
    for d in range(2):
        pl.when(has[d])(lambda: signal({"row": targets[d]}))
    pl.when(has[0] & has[1])(lambda: pl.semaphore_wait(barrier, 5))
    pl.when(jnp.logical_not(has[0] & has[1]))(lambda: pl.semaphore_wait(barrier, 4))

    for c in order:
        for d in range(2):
            pl.when(has[d])(lambda: side(d, c).start())
    pair().start()
    local = pltpu.make_async_copy(own, band.at[2], own_sem)
    local.start()

    passes = (odd == 0, odd == 1)

    for c in order:
        for d in range(2):

            @pl.when(takes[d])
            def _():
                side(d, c).wait_recv()
                near_out(d, c).start()

            pl.when(takes[d] & passes[d])(lambda: passed(mine + c).start())

    for c in order:
        for d in range(2):
            pl.when(takes[d])(lambda: near_in(d, c).wait_recv())
            pl.when(takes[d] & passes[d])(lambda: passed(other + c).start())

    passing = ((odd == 0) & takes[0]) | ((odd == 1) & takes[1])
    passed_to = ((odd == 1) & takes[0]) | ((odd == 0) & takes[1])

    @pl.when(passed_to)
    def _():
        for c in range(2 * half):
            passed(c).wait_recv()

    local.wait()
    pair().wait_recv()
    pair().wait_send()
    for c in order:
        for d in range(2):
            pl.when(has[d])(lambda: side(d, c).wait_send())
            pl.when(takes[d])(lambda: near_out(d, c).wait_send())

    @pl.when(passing)
    def _():
        for c in range(2 * half):
            passed(c).wait_send()


def gathered(p_tiles, rows, groups):
    fine_rows = p_tiles.shape[0]
    half = fine_rows // 2
    vmem = pl.BlockSpec(memory_space=pltpu.VMEM)
    dma = pltpu.SemaphoreType.DMA
    return pl.pallas_call(
        functools.partial(gather_kernel, rows, groups),
        out_shape=jax.ShapeDtypeStruct((5,) + p_tiles.shape, p_tiles.dtype),
        in_specs=[vmem],
        out_specs=vmem,
        scratch_shapes=[
            dma((2, 2, half)),
            dma((2, 2, half)),
            dma((2,)),
            dma((2, fine_rows)),
            dma,
        ],
        compiler_params=pltpu.CompilerParams(
            collective_id=1, has_side_effects=True, vmem_limit_bytes=16 * 1024 * 1024
        ),
    )(p_tiles)


def body(a_tiles, a_cols, p_tiles, p_cols, c_cols):
    fine_rows = a_tiles.shape[0]
    coarse_rows = fine_rows // RATIO
    tile = a_tiles.shape[-1]
    kc = c_cols.shape[1]
    chunks = lax.axis_size("grp")
    position = lax.axis_index("row")
    band = gathered(p_tiles, lax.axis_size("row"), chunks)
    band = band.reshape((5 * fine_rows,) + p_tiles.shape[1:])
    center, codes, scales = local_products(
        a_tiles, a_cols, band, p_cols, c_cols, position, chunks
    )
    out = exchange(center, codes, scales, lax.axis_size("row"))
    return out.reshape(coarse_rows, kc // chunks, tile, tile)


def solution(mesh):
    return jax.shard_map(
        body,
        mesh=mesh,
        in_specs=(
            P("row", "grp", None, None, None),
            P("row", "grp", None),
            P("row", None, None, None),
            P(),
            P(),
        ),
        out_specs=P("row", "grp", None, None),
        check_vma=False,
    )
```

```python
import functools

import jax
import jax.numpy as jnp
from jax import lax
from jax.experimental import pallas as pl
from jax.experimental.pallas import tpu as pltpu
from jax.sharding import PartitionSpec as P

RATIO = 2
REACH = 2


LEVELS = 32767.0


def encoded(value):
    most = jnp.maximum(jnp.max(jnp.abs(value), axis=0, keepdims=True), 2e-34)
    code = jnp.round(value * (LEVELS / most)).astype(jnp.int32).astype(jnp.int16)
    return code, most * (1.0 / LEVELS)


def decoded(code, scale):
    return code.astype(jnp.int32).astype(jnp.float32) * scale


def product_kernel(
    sizes,
    where,
    a_cols,
    p_cols,
    a_ref,
    band_ref,
    halves,
    left_ref,
    slot_of,
    links,
    sums,
):
    fine_rows, slots, kp, tile = sizes
    coarse_rows = fine_rows // RATIO
    window = (2 * (REACH + 2) + 1) * coarse_rows
    entries = slots * kp
    empty = fine_rows * entries
    position = where[0]
    first_row = position * fine_rows
    band_start = first_row - REACH * fine_rows
    window_start = (position - REACH - 2) * coarse_rows
    base_coarse = (position - 1) * coarse_rows
    halves[empty] = jnp.zeros((2 * tile, tile), jnp.bfloat16)
    sums[entries] = jnp.zeros((tile, tile), jnp.float32)

    @pl.loop(0, fine_rows * window, unroll=8)
    def _(n):
        slot_of[n] = empty

    for c in range(3 * coarse_rows):
        links[fine_rows * kp + c] = 0

    @pl.loop(0, fine_rows)
    def _(i):
        for q in range(kp):
            left_ref[i * kp + q] = band_ref[(REACH * fine_rows + i) * kp + q].T
            e = i * kp + q
            c = fine_rows * kp + p_cols[q, first_row + i] - base_coarse
            links[e] = links[c]
            links[c] = e + 1
        for s in range(slots):
            j = a_cols[s, 0, i]
            local = (j - band_start) * kp
            right = jnp.concatenate([band_ref[local + p] for p in range(kp)], axis=1)
            prod = jnp.dot(a_ref[i * slots + s], right, preferred_element_type=jnp.float32)
            for p in range(kp):
                at = i * window + p_cols[p, j] - window_start
                before = jnp.minimum(slot_of[at] - i * entries, entries)
                now = s * kp + p
                slot_of[at] = i * entries + now
                value = sums[before] + prod[:, p * tile : (p + 1) * tile]
                sums[now] = value
                high = value.astype(jnp.bfloat16)
                halves[i * entries + now, :tile] = high
                halves[i * entries + now, tile:] = (
                    value - high.astype(jnp.float32)
                ).astype(jnp.bfloat16)


def local_products(a_tiles, a_cols, band, p_cols, position):
    fine_rows, _, slots, tile, _ = a_tiles.shape
    kp = band.shape[1]
    coarse_rows = fine_rows // RATIO
    window = (2 * (REACH + 2) + 1) * coarse_rows
    entries = slots * kp
    smem = pl.BlockSpec(memory_space=pltpu.SMEM)
    vmem = pl.BlockSpec(memory_space=pltpu.VMEM)
    return pl.pallas_call(
        functools.partial(product_kernel, (fine_rows, slots, kp, tile)),
        out_shape=[
            jax.ShapeDtypeStruct((fine_rows * entries + 1, 2 * tile, tile), jnp.bfloat16),
            jax.ShapeDtypeStruct((fine_rows * kp, tile, tile), jnp.bfloat16),
            jax.ShapeDtypeStruct((fine_rows * window,), jnp.int32),
            jax.ShapeDtypeStruct((fine_rows * kp + 3 * coarse_rows,), jnp.int32),
        ],
        in_specs=[smem] * 3 + [vmem] * 2,
        out_specs=[vmem] * 2 + [smem] * 2,
        scratch_shapes=[pltpu.VMEM((entries + 1, tile, tile), jnp.float32)],
        compiler_params=pltpu.CompilerParams(vmem_limit_bytes=28 * 1024 * 1024),
    )(
        position.reshape(1),
        a_cols.T,
        p_cols.T,
        a_tiles.reshape(-1, tile, tile),
        band.reshape(-1, tile, tile),
    )


def exchange_kernel(
    sizes,
    p_cols,
    c_cols,
    slot_of,
    links,
    halves,
    left_ref,
    out,
    runs,
    center,
    codes,
    scales,
    got_codes,
    got_scales,
    sent_codes,
    sent_scales,
    peer_codes,
    peer_scales,
    side_sems,
    side_scale_sems,
    peer_sems,
    peer_scale_sems,
):
    fine_rows, kp, kc, tile, rows, groups = sizes
    r = lax.axis_index("row")
    g = lax.axis_index("grp")
    coarse_rows = fine_rows // RATIO
    window = (2 * (REACH + 2) + 1) * coarse_rows
    window_start = (r - REACH - 2) * coarse_rows
    first_row = r * fine_rows
    share = kc // groups
    half = share // 2
    members = half * coarse_rows
    odd = lax.rem(r, 2)
    toward = 2 * odd - 1
    outer, inner = r + toward, r - toward
    has_outer = (outer >= 0) & (outer < rows)
    g_odd = lax.rem(g, 2)
    g_high = lax.rem(g // 2, 2)
    near = (g + 1 - 2 * g_odd, g + 2 - 4 * g_high)
    far = near[0] + 2 - 4 * g_high
    wanted = ((far, far), (near[0], near[1]), (near[1], near[0]), (g, g))
    steps = len(wanted)
    barrier = pltpu.get_barrier_semaphore()
    mesh_type = pl.DeviceIdType.MESH

    def signal(to):
        pl.semaphore_signal(barrier, inc=1, device_id=to, device_id_type=mesh_type)

    signal({"row": inner})
    signal({"grp": near[0]})
    signal({"grp": near[1]})
    pl.when(has_outer)(lambda: signal({"row": outer}))

    def copy(src, dst, sems, at, to):
        return pltpu.make_async_remote_copy(
            src_ref=src,
            dst_ref=dst,
            send_sem=sems.at[(0,) + at],
            recv_sem=sems.at[(1,) + at],
            device_id=to,
            device_id_type=mesh_type,
        )

    def side_copies(pos, t):
        to = {"row": inner if pos else outer}
        return (
            copy(scales.at[pos, t], got_scales.at[pos, t], side_scale_sems, (pos, t), to),
            copy(codes.at[pos, t], got_codes.at[pos, t], side_sems, (pos, t), to),
        )

    def peer_copies(n, t):
        to = {"grp": near[n]}
        return (
            copy(
                sent_scales.at[n, t], peer_scales.at[n, t], peer_scale_sems, (n, t), to
            ),
            copy(sent_codes.at[n, t], peer_codes.at[n, t], peer_sems, (n, t), to),
        )

    def start(copies):
        for one in copies:
            one.start()

    def arrive(copies):
        for one in copies:
            one.wait_recv()

    def leave(copies):
        for one in copies:
            one.wait_send()

    runs[0] = jnp.zeros(runs.shape[1:], jnp.float32)

    @pl.when(jnp.logical_not(has_outer))
    def _():
        got_scales[0] = jnp.zeros(got_scales.shape[1:], jnp.float32)

        @pl.loop(0, 2 * members)
        def _(m):
            for t in range(steps):
                got_codes[0, t, m] = jnp.zeros((tile, tile), jnp.int16)

    def compute(t):
        @pl.loop(0, fine_rows)
        def _(i):
            for q in range(kp):
                e = i * kp + q
                c = p_cols[q, first_row + i]
                own = left_ref[e]
                left = jnp.concatenate([own, own], axis=1)
                parts = []
                for n in range(share):
                    k = wanted[t][n // half] * share + n
                    w = jnp.clip(c_cols[k, c] - window_start, 0, window - 1)
                    parts.append(halves[slot_of[i * window + w]])
                prod = jnp.dot(
                    left, jnp.concatenate(parts, axis=1), preferred_element_type=jnp.float32
                )
                before = links[e]
                for n in range(share):
                    runs[e + 1, n] = runs[before, n] + prod[:, n * tile : (n + 1) * tile]

    def last(block, c):
        return links[fine_rows * kp + block * coarse_rows + c]

    def encode(t, pos):
        block = 2 * (1 - odd) if pos else 2 * odd

        @pl.loop(0, coarse_rows)
        def _(c):
            at = last(block, c)
            for n in range(share):
                m = n * coarse_rows + c
                code, scale = encoded(runs[at, n])
                codes[pos, t, m] = code
                scales[pos, t, pl.ds(m, 1)] = scale

    def keep(t):
        @pl.loop(0, coarse_rows)
        def _(c):
            at = last(1, c)
            for n in range(share):
                center[t, n * coarse_rows + c] = runs[at, n]

    def made(t):
        compute(t)
        encode(t, 0)
        if t == 0:
            pl.when(has_outer)(lambda: pl.semaphore_wait(barrier, 4))
            pl.when(jnp.logical_not(has_outer))(lambda: pl.semaphore_wait(barrier, 3))
        pl.when(has_outer)(lambda: start(side_copies(0, t)))
        encode(t, 1)
        start(side_copies(1, t))
        keep(t)

    def summed(t, m):
        value = center[t, m]
        for pos in range(2):
            value += decoded(got_codes[pos, t, m], got_scales[pos, t, pl.ds(m, 1)])
        return value

    def peer(n, t, m):
        return decoded(peer_codes[n, t, m], peer_scales[n, t, pl.ds(m, 1)])

    def come(t):
        pl.when(has_outer)(lambda: arrive(side_copies(0, t)))
        arrive(side_copies(1, t))

    def forward(t):
        come(t)
        if t == 2:
            for n in range(2):
                arrive(peer_copies(n, 0))
        for part in range(2):
            n = 1 - part if t == 2 else part

            @pl.loop(0, members)
            def _(m):
                value = summed(t, part * members + m)
                if t == 2:
                    value += peer(part, 0, m)
                code, scale = encoded(value)
                sent_codes[n, t, m] = code
                sent_scales[n, t, pl.ds(m, 1)] = scale

            start(peer_copies(n, t))

    def finish(t):
        come(t)
        for n in range(2):
            arrive(peer_copies(n, 1))
            arrive(peer_copies(n, 2))

        @pl.loop(0, coarse_rows)
        def _(c):
            for n in range(share):
                part = n // half
                m = (n - part * half) * coarse_rows + c
                value = summed(t, n * coarse_rows + c)
                out[c * share + n] = value + peer(part, 1, m) + peer(1 - part, 2, m)

    made(0)
    made(1)
    made(2)
    forward(0)
    made(3)
    forward(1)
    forward(2)
    finish(3)
    for t in range(steps):
        pl.when(has_outer)(lambda: leave(side_copies(0, t)))
        leave(side_copies(1, t))
    for t in range(steps - 1):
        for n in range(2):
            leave(peer_copies(n, t))


def exchange(halves, left, slot_of, links, p_cols, c_cols, rows, groups):
    _, tile = halves.shape[1:]
    kp = p_cols.shape[1]
    kc = c_cols.shape[1]
    fine_rows = left.shape[0] // kp
    coarse_rows = fine_rows // RATIO
    share = kc // groups
    members = share * coarse_rows
    steps = 4
    smem = pl.BlockSpec(memory_space=pltpu.SMEM)
    vmem = pl.BlockSpec(memory_space=pltpu.VMEM)
    dma = pltpu.SemaphoreType.DMA

    def tiles(*lead):
        return [
            pltpu.VMEM(lead + (tile, tile), jnp.int16),
            pltpu.VMEM(lead + (tile,), jnp.float32),
        ]

    return pl.pallas_call(
        functools.partial(exchange_kernel, (fine_rows, kp, kc, tile, rows, groups)),
        out_shape=jax.ShapeDtypeStruct((members, tile, tile), jnp.float32),
        in_specs=[smem] * 4 + [vmem] * 2,
        out_specs=vmem,
        scratch_shapes=[
            pltpu.VMEM((fine_rows * kp + 1, share, tile, tile), jnp.float32),
            pltpu.VMEM((steps, members, tile, tile), jnp.float32),
            *tiles(2, steps, members),
            *tiles(2, steps, members),
            *tiles(2, steps - 1, members // 2),
            *tiles(2, steps - 1, members // 2),
            dma((2, 2, steps)),
            dma((2, 2, steps)),
            dma((2, 2, steps - 1)),
            dma((2, 2, steps - 1)),
        ],
        compiler_params=pltpu.CompilerParams(
            collective_id=0, has_side_effects=True, vmem_limit_bytes=28 * 1024 * 1024
        ),
    )(p_cols.T, c_cols.T, slot_of, links, halves, left)


def gather_kernel(
    rows,
    groups,
    own,
    band,
    side_sems,
    near_sems,
    pair_sems,
    pass_sems,
    own_sem,
):
    r = lax.axis_index("row")
    g = lax.axis_index("grp")
    odd = lax.rem(r, 2)
    partner = r + 1 - 2 * odd
    has = (r >= 2, r < rows - 2)
    takes = (r < rows - 2, r >= 2)
    blocks = (4, 0)
    targets = (r - 2, r + 2)
    g_odd = lax.rem(g, 2)
    g_high = lax.rem(g // 2, 2)
    near = (g + 1 - 2 * g_odd, g + 2 - 4 * g_high)
    half = own.shape[0] // 2
    parity = lax.rem(g_odd + g_high, 2)
    mine = parity * half
    other = (1 - parity) * half
    barrier = pltpu.get_barrier_semaphore()
    mesh_type = pl.DeviceIdType.MESH
    turn = half // 2
    order = [n * turn + c for c in range(turn) for n in range(2)]

    def copy(src, dst, send, recv, to):
        return pltpu.make_async_remote_copy(
            src_ref=src,
            dst_ref=dst,
            send_sem=send,
            recv_sem=recv,
            device_id=to,
            device_id_type=mesh_type,
        )

    def side(d, c):
        at = mine + c
        return copy(
            own.at[at],
            band.at[blocks[d], at],
            side_sems.at[0, d, c],
            side_sems.at[1, d, c],
            {"row": targets[d]},
        )

    def near_out(d, c):
        at = mine + c
        return copy(
            band.at[blocks[d], at],
            band.at[blocks[d], at],
            near_sems.at[0, d, c],
            near_sems.at[1, d, c],
            {"grp": near[c // turn]},
        )

    def near_in(d, c):
        at = other + c
        return copy(
            band.at[blocks[d], at],
            band.at[blocks[d], at],
            near_sems.at[0, d, c],
            near_sems.at[1, d, c],
            {"grp": near[c // turn]},
        )

    def pair():
        return copy(
            own, band.at[1 + 2 * odd], pair_sems.at[0], pair_sems.at[1], {"row": partner}
        )

    def passed(at):
        return copy(
            band.at[4 - 4 * odd, at],
            band.at[3 - 2 * odd, at],
            pass_sems.at[0, at],
            pass_sems.at[1, at],
            {"row": partner},
        )

    def signal(to):
        pl.semaphore_signal(barrier, inc=1, device_id=to, device_id_type=mesh_type)

    signal({"row": partner})
    signal({"grp": near[0]})
    signal({"grp": near[1]})
    for d in range(2):
        pl.when(has[d])(lambda: signal({"row": targets[d]}))
    pl.when(has[0] & has[1])(lambda: pl.semaphore_wait(barrier, 5))
    pl.when(jnp.logical_not(has[0] & has[1]))(lambda: pl.semaphore_wait(barrier, 4))

    for c in order:
        for d in range(2):
            pl.when(has[d])(lambda: side(d, c).start())
    pair().start()
    local = pltpu.make_async_copy(own, band.at[2], own_sem)
    local.start()

    passes = (odd == 0, odd == 1)

    for c in order:
        for d in range(2):

            @pl.when(takes[d])
            def _():
                side(d, c).wait_recv()
                near_out(d, c).start()

            pl.when(takes[d] & passes[d])(lambda: passed(mine + c).start())

    for c in order:
        for d in range(2):
            pl.when(takes[d])(lambda: near_in(d, c).wait_recv())
            pl.when(takes[d] & passes[d])(lambda: passed(other + c).start())

    passing = ((odd == 0) & takes[0]) | ((odd == 1) & takes[1])
    passed_to = ((odd == 1) & takes[0]) | ((odd == 0) & takes[1])

    @pl.when(passed_to)
    def _():
        for c in range(2 * half):
            passed(c).wait_recv()

    local.wait()
    pair().wait_recv()
    pair().wait_send()
    for c in order:
        for d in range(2):
            pl.when(has[d])(lambda: side(d, c).wait_send())
            pl.when(takes[d])(lambda: near_out(d, c).wait_send())

    @pl.when(passing)
    def _():
        for c in range(2 * half):
            passed(c).wait_send()


def gathered(p_tiles, rows, groups):
    fine_rows = p_tiles.shape[0]
    half = fine_rows // 2
    vmem = pl.BlockSpec(memory_space=pltpu.VMEM)
    dma = pltpu.SemaphoreType.DMA
    return pl.pallas_call(
        functools.partial(gather_kernel, rows, groups),
        out_shape=jax.ShapeDtypeStruct((5,) + p_tiles.shape, p_tiles.dtype),
        in_specs=[vmem],
        out_specs=vmem,
        scratch_shapes=[
            dma((2, 2, half)),
            dma((2, 2, half)),
            dma((2,)),
            dma((2, fine_rows)),
            dma,
        ],
        compiler_params=pltpu.CompilerParams(
            collective_id=1, has_side_effects=True, vmem_limit_bytes=16 * 1024 * 1024
        ),
    )(p_tiles)


def body(a_tiles, a_cols, p_tiles, p_cols, c_cols):
    fine_rows = a_tiles.shape[0]
    coarse_rows = fine_rows // RATIO
    tile = a_tiles.shape[-1]
    kc = c_cols.shape[1]
    chunks = lax.axis_size("grp")
    position = lax.axis_index("row")
    band = gathered(p_tiles, lax.axis_size("row"), chunks)
    band = band.reshape((5 * fine_rows,) + p_tiles.shape[1:])
    halves, left, slot_of, links = local_products(a_tiles, a_cols, band, p_cols, position)
    out = exchange(halves, left, slot_of, links, p_cols, c_cols, lax.axis_size("row"), chunks)
    return out.reshape(coarse_rows, kc // chunks, tile, tile)


def solution(mesh):
    return jax.shard_map(
        body,
        mesh=mesh,
        in_specs=(
            P("row", "grp", None, None, None),
            P("row", "grp", None),
            P("row", None, None, None),
            P(),
            P(),
        ),
        out_specs=P("row", "grp", None, None),
        check_vma=False,
    )
```

```python
import functools

import jax
import jax.numpy as jnp
from jax import lax
from jax.experimental import pallas as pl
from jax.experimental.pallas import tpu as pltpu
from jax.sharding import PartitionSpec as P

RATIO = 2
REACH = 2


LEVELS = 32767.0


def encoded(value):
    most = jnp.maximum(jnp.max(jnp.abs(value), axis=0, keepdims=True), 2e-34)
    code = jnp.round(value * (LEVELS / most)).astype(jnp.int32).astype(jnp.int16)
    return code, most * (1.0 / LEVELS)


def decoded(code, scale):
    return code.astype(jnp.int32).astype(jnp.float32) * scale


def product_kernel(
    sizes,
    where,
    a_cols,
    p_cols,
    a_ref,
    band_ref,
    halves,
    left_ref,
    slot_of,
    links,
    sums,
):
    fine_rows, slots, kp, tile = sizes
    coarse_rows = fine_rows // RATIO
    window = (2 * (REACH + 2) + 1) * coarse_rows
    entries = slots * kp
    empty = fine_rows * entries
    position = where[0]
    first_row = position * fine_rows
    band_start = first_row - REACH * fine_rows
    window_start = (position - REACH - 2) * coarse_rows
    base_coarse = (position - 1) * coarse_rows
    halves[empty] = jnp.zeros((2 * tile, tile), jnp.bfloat16)
    sums[entries] = jnp.zeros((tile, tile), jnp.float32)

    @pl.loop(0, fine_rows * window, unroll=8)
    def _(n):
        slot_of[n] = empty

    for c in range(3 * coarse_rows):
        links[fine_rows * kp + c] = 0

    @pl.loop(0, fine_rows)
    def _(i):
        for q in range(kp):
            left_ref[i * kp + q] = band_ref[(REACH * fine_rows + i) * kp + q].T
            e = i * kp + q
            c = fine_rows * kp + p_cols[q, first_row + i] - base_coarse
            links[e] = links[c]
            links[c] = e + 1
        for s in range(slots):
            j = a_cols[s, 0, i]
            local = (j - band_start) * kp
            right = jnp.concatenate([band_ref[local + p] for p in range(kp)], axis=1)
            prod = jnp.dot(a_ref[i * slots + s], right, preferred_element_type=jnp.float32)
            for p in range(kp):
                at = i * window + p_cols[p, j] - window_start
                before = jnp.minimum(slot_of[at] - i * entries, entries)
                now = s * kp + p
                slot_of[at] = i * entries + now
                value = sums[before] + prod[:, p * tile : (p + 1) * tile]
                sums[now] = value
                high = value.astype(jnp.bfloat16)
                halves[i * entries + now, :tile] = high
                halves[i * entries + now, tile:] = (
                    value - high.astype(jnp.float32)
                ).astype(jnp.bfloat16)


def local_products(a_tiles, a_cols, band, p_cols, position):
    fine_rows, _, slots, tile, _ = a_tiles.shape
    kp = band.shape[1]
    coarse_rows = fine_rows // RATIO
    window = (2 * (REACH + 2) + 1) * coarse_rows
    entries = slots * kp
    smem = pl.BlockSpec(memory_space=pltpu.SMEM)
    vmem = pl.BlockSpec(memory_space=pltpu.VMEM)
    return pl.pallas_call(
        functools.partial(product_kernel, (fine_rows, slots, kp, tile)),
        out_shape=[
            jax.ShapeDtypeStruct((fine_rows * entries + 1, 2 * tile, tile), jnp.bfloat16),
            jax.ShapeDtypeStruct((fine_rows * kp, tile, tile), jnp.bfloat16),
            jax.ShapeDtypeStruct((fine_rows * window,), jnp.int32),
            jax.ShapeDtypeStruct((fine_rows * kp + 3 * coarse_rows,), jnp.int32),
        ],
        in_specs=[smem] * 3 + [vmem] * 2,
        out_specs=[vmem] * 2 + [smem] * 2,
        scratch_shapes=[pltpu.VMEM((entries + 1, tile, tile), jnp.float32)],
        compiler_params=pltpu.CompilerParams(vmem_limit_bytes=28 * 1024 * 1024),
    )(
        position.reshape(1),
        a_cols.T,
        p_cols.T,
        a_tiles.reshape(-1, tile, tile),
        band.reshape(-1, tile, tile),
    )


def exchange_kernel(
    sizes,
    p_cols,
    c_cols,
    slot_of,
    links,
    halves,
    left_ref,
    out,
    runs,
    center,
    codes,
    scales,
    got_codes,
    got_scales,
    sent_codes,
    sent_scales,
    peer_codes,
    peer_scales,
    side_sems,
    side_scale_sems,
    peer_sems,
    peer_scale_sems,
):
    fine_rows, kp, kc, tile, rows, groups = sizes
    r = lax.axis_index("row")
    g = lax.axis_index("grp")
    coarse_rows = fine_rows // RATIO
    window = (2 * (REACH + 2) + 1) * coarse_rows
    window_start = (r - REACH - 2) * coarse_rows
    first_row = r * fine_rows
    share = kc // groups
    half = share // 2
    members = half * coarse_rows
    pieces = min(fine_rows, members) // 2
    size = members // pieces
    pace = fine_rows // pieces
    odd = lax.rem(r, 2)
    toward = 2 * odd - 1
    outer, inner = r + toward, r - toward
    has_outer = (outer >= 0) & (outer < rows)
    g_odd = lax.rem(g, 2)
    g_high = lax.rem(g // 2, 2)
    near = (g + 1 - 2 * g_odd, g + 2 - 4 * g_high)
    far = near[0] + 2 - 4 * g_high
    wanted = ((far, far), (near[0], near[1]), (near[1], near[0]), (g, g))
    steps = len(wanted)
    barrier = pltpu.get_barrier_semaphore()
    mesh_type = pl.DeviceIdType.MESH

    def signal(to):
        pl.semaphore_signal(barrier, inc=1, device_id=to, device_id_type=mesh_type)

    signal({"row": inner})
    signal({"grp": near[0]})
    signal({"grp": near[1]})
    pl.when(has_outer)(lambda: signal({"row": outer}))

    def copy(src, dst, sems, at, to):
        return pltpu.make_async_remote_copy(
            src_ref=src,
            dst_ref=dst,
            send_sem=sems.at[(0,) + at],
            recv_sem=sems.at[(1,) + at],
            device_id=to,
            device_id_type=mesh_type,
        )

    def side_scales(pos, t):
        to = {"row": inner if pos else outer}
        return (copy(scales.at[pos, t], got_scales.at[pos, t], side_scale_sems, (pos, t), to),)

    def side_piece(pos, t, part, n):
        to = {"row": inner if pos else outer}
        some = pl.ds(part * members + n * size, size)
        at = (pos, t, part, n)
        return (copy(codes.at[pos, t, some], got_codes.at[pos, t, some], side_sems, at, to),)

    def peer_piece(part, t, n):
        to = {"grp": near[part]}
        some = pl.ds(n * size, size)
        at = (part, t, n)
        return (
            copy(
                sent_scales.at[part, t, some],
                peer_scales.at[part, t, some],
                peer_scale_sems,
                at,
                to,
            ),
            copy(
                sent_codes.at[part, t, some],
                peer_codes.at[part, t, some],
                peer_sems,
                at,
                to,
            ),
        )

    def start(copies):
        for one in copies:
            one.start()

    def arrive(copies):
        for one in copies:
            one.wait_recv()

    def leave(copies):
        for one in copies:
            one.wait_send()

    runs[0] = jnp.zeros(runs.shape[1:], jnp.float32)

    @pl.when(jnp.logical_not(has_outer))
    def _():
        got_scales[0] = jnp.zeros(got_scales.shape[1:], jnp.float32)

        @pl.loop(0, 2 * members)
        def _(m):
            for t in range(steps):
                got_codes[0, t, m] = jnp.zeros((tile, tile), jnp.int16)

    def compute(t, i):
        for q in range(kp):
            e = i * kp + q
            c = p_cols[q, first_row + i]
            own = left_ref[e]
            left = jnp.concatenate([own, own], axis=1)
            parts = []
            for n in range(share):
                k = wanted[t][n // half] * share + n
                w = jnp.clip(c_cols[k, c] - window_start, 0, window - 1)
                parts.append(halves[slot_of[i * window + w]])
            prod = jnp.dot(
                left, jnp.concatenate(parts, axis=1), preferred_element_type=jnp.float32
            )
            before = links[e]
            for n in range(share):
                runs[e + 1, n] = runs[before, n] + prod[:, n * tile : (n + 1) * tile]

    def last(block, c):
        return links[fine_rows * kp + block * coarse_rows + c]

    def encode(t, pos):
        block = 2 * (1 - odd) if pos else 2 * odd

        @pl.loop(0, coarse_rows)
        def _(c):
            at = last(block, c)
            for n in range(share):
                m = n * coarse_rows + c
                code, scale = encoded(runs[at, n])
                codes[pos, t, m] = code
                scales[pos, t, m] = scale

    def keep(t):
        @pl.loop(0, coarse_rows)
        def _(c):
            at = last(1, c)
            for n in range(share):
                center[t, n * coarse_rows + c] = runs[at, n]

    def each_piece(act, pos, t):
        for n in range(pieces):
            for part in range(2):
                act(side_piece(pos, t, part, n))

    def send(t):
        encode(t, 0)
        if t == 0:
            pl.when(has_outer)(lambda: pl.semaphore_wait(barrier, 4))
            pl.when(jnp.logical_not(has_outer))(lambda: pl.semaphore_wait(barrier, 3))

        @pl.when(has_outer)
        def _():
            start(side_scales(0, t))
            each_piece(start, 0, t)

        encode(t, 1)
        start(side_scales(1, t))
        each_piece(start, 1, t)
        keep(t)

    def summed(t, m):
        value = center[t, m]
        for pos in range(2):
            value += decoded(got_codes[pos, t, m], got_scales[pos, t, m])
        return value

    def peer(n, t, m):
        return decoded(peer_codes[n, t, m], peer_scales[n, t, m])

    def open_step(t):
        pl.when(has_outer)(lambda: arrive(side_scales(0, t)))
        arrive(side_scales(1, t))

    def come(t, part, n):
        pl.when(has_outer)(lambda: arrive(side_piece(0, t, part, n)))
        arrive(side_piece(1, t, part, n))

    def forward(t, n):
        for part in range(2):
            to = 1 - part if t == 2 else part
            come(t, part, n)
            if t == 2:
                arrive(peer_piece(part, 0, n))
            for u in range(size):
                m = n * size + u
                value = summed(t, part * members + m)
                if t == 2:
                    value += peer(part, 0, m)
                code, scale = encoded(value)
                sent_codes[to, t, m] = code
                sent_scales[to, t, m] = scale
            start(peer_piece(to, t, n))

    def finish(t, n):
        for part in range(2):
            come(t, part, n)
            arrive(peer_piece(part, 1, n))
            arrive(peer_piece(1 - part, 2, n))
            for u in range(size):
                m = n * size + u
                c = lax.rem(m, coarse_rows)
                k = part * half + m // coarse_rows
                value = summed(t, part * members + m)
                out[c * share + k] = value + peer(part, 1, m) + peer(1 - part, 2, m)

    for t in range(2):
        pl.loop(0, fine_rows)(lambda i: compute(t, i))
        send(t)
    for t in range(2):
        open_step(t)

        @pl.loop(0, pieces)
        def _(n):
            for u in range(pace):
                compute(t + 2, n * pace + u)
            forward(t, n)

        send(t + 2)
    open_step(2)
    pl.loop(0, pieces)(lambda n: forward(2, n))
    open_step(3)
    pl.loop(0, pieces)(lambda n: finish(3, n))
    for t in range(steps):

        @pl.when(has_outer)
        def _():
            leave(side_scales(0, t))
            each_piece(leave, 0, t)

        leave(side_scales(1, t))
        each_piece(leave, 1, t)
    for t in range(steps - 1):
        for part in range(2):
            for n in range(pieces):
                leave(peer_piece(part, t, n))


def exchange(halves, left, slot_of, links, p_cols, c_cols, rows, groups):
    _, tile = halves.shape[1:]
    kp = p_cols.shape[1]
    kc = c_cols.shape[1]
    fine_rows = left.shape[0] // kp
    coarse_rows = fine_rows // RATIO
    share = kc // groups
    members = share * coarse_rows
    pieces = min(fine_rows, members // 2) // 2
    steps = 4
    smem = pl.BlockSpec(memory_space=pltpu.SMEM)
    vmem = pl.BlockSpec(memory_space=pltpu.VMEM)
    dma = pltpu.SemaphoreType.DMA

    def tiles(*lead):
        return [
            pltpu.VMEM(lead + (tile, tile), jnp.int16),
            pltpu.VMEM(lead + (1, tile), jnp.float32),
        ]

    return pl.pallas_call(
        functools.partial(exchange_kernel, (fine_rows, kp, kc, tile, rows, groups)),
        out_shape=jax.ShapeDtypeStruct((members, tile, tile), jnp.float32),
        in_specs=[smem] * 4 + [vmem] * 2,
        out_specs=vmem,
        scratch_shapes=[
            pltpu.VMEM((fine_rows * kp + 1, share, tile, tile), jnp.float32),
            pltpu.VMEM((steps, members, tile, tile), jnp.float32),
            *tiles(2, steps, members),
            *tiles(2, steps, members),
            *tiles(2, steps - 1, members // 2),
            *tiles(2, steps - 1, members // 2),
            dma((2, 2, steps, 2, pieces)),
            dma((2, 2, steps)),
            dma((2, 2, steps - 1, pieces)),
            dma((2, 2, steps - 1, pieces)),
        ],
        compiler_params=pltpu.CompilerParams(
            collective_id=0, has_side_effects=True, vmem_limit_bytes=28 * 1024 * 1024
        ),
    )(p_cols.T, c_cols.T, slot_of, links, halves, left)


def gather_kernel(
    rows,
    passing,
    own,
    band,
    side_sends,
    side_comes,
    near_sends,
    near_comes,
    pair_sems,
    pass_sems,
    own_sem,
):
    r = lax.axis_index("row")
    g = lax.axis_index("grp")
    odd = lax.rem(r, 2)
    partner = r + 1 - 2 * odd
    has = (r >= 2, r < rows - 2)
    handed, kept = odd, 1 - odd
    takes_handed = jnp.where(odd == 0, r < rows - 2, r >= 2)
    takes_kept = jnp.where(odd == 0, r >= 2, r < rows - 2)
    g_odd = lax.rem(g, 2)
    g_high = lax.rem(g // 2, 2)
    near = (g + 1 - 2 * g_odd, g + 2 - 4 * g_high)
    parity = lax.rem(g_odd + g_high, 2)
    tiles = own.shape[0]
    direct = tiles - passing
    mine = parity * direct
    other = (1 - parity) * direct
    barrier = pltpu.get_barrier_semaphore()
    mesh_type = pl.DeviceIdType.MESH
    local = pltpu.make_async_copy(own, band.at[2], own_sem)
    local.start()

    def copy(src, dst, send, recv, to):
        return pltpu.make_async_remote_copy(
            src_ref=src,
            dst_ref=dst,
            send_sem=send,
            recv_sem=recv,
            device_id=to,
            device_id_type=mesh_type,
        )

    def place(n):
        return mine + n if n < passing else n

    def side(d, at, size, n):
        part = pl.ds(at, size)
        return copy(
            band.at[2, part],
            band.at[4 - 4 * d, part],
            side_sends.at[d],
            side_comes.at[d, n],
            {"row": r - 2 + 4 * d},
        )

    def near_copy(d, at, size, n):
        ref = band.at[4 - 4 * d, pl.ds(at, size)]
        to = {"grp": near[n % 2]}
        return copy(ref, ref, near_sends.at[d], near_comes.at[d, n], to)

    def pair():
        return copy(
            band.at[2],
            band.at[1 + 2 * odd],
            pair_sems.at[0],
            pair_sems.at[1],
            {"row": partner},
        )

    def passed(at, size):
        part = pl.ds(at, size)
        return copy(
            band.at[4 - 4 * odd, part],
            band.at[3 - 2 * odd, part],
            pass_sems.at[0],
            pass_sems.at[1],
            {"row": partner},
        )

    def signal(to):
        pl.semaphore_signal(barrier, inc=1, device_id=to, device_id_type=mesh_type)

    signal({"row": partner})
    signal({"grp": near[0]})
    signal({"grp": near[1]})
    for d in range(2):
        pl.when(has[d])(lambda: signal({"row": r - 2 + 4 * d}))
    local.wait()
    pl.when(has[0] & has[1])(lambda: pl.semaphore_wait(barrier, 5))
    pl.when(jnp.logical_not(has[0] & has[1]))(lambda: pl.semaphore_wait(barrier, 4))

    for d in range(2):

        @pl.when(has[d])
        def _():
            for n in range(direct):
                side(d, place(n), 1, n).start()

    pair().start()

    for n in range(direct):

        @pl.when(takes_handed)
        def _():
            side(handed, place(n), 1, n).wait_recv()
            if n < passing:
                near_copy(handed, mine + n, 1, n).start()
            passed(place(n), 1).start()

        if n < passing:

            @pl.when(takes_kept)
            def _():
                side(kept, place(n), 1, n).wait_recv()
                near_copy(kept, mine + n, 1, n).start()

    @pl.when(takes_handed)
    def _():
        for n in range(passing):
            near_copy(handed, other + n, 1, n).wait_recv()
            passed(other + n, 1).start()

    @pl.when(takes_kept)
    def _():
        for n in range(passing, direct):
            side(kept, place(n), 1, n).wait_recv()
        for n in range(passing):
            near_copy(kept, other + n, 1, n).wait_recv()
        passed(0, tiles).wait_recv()
        near_copy(kept, mine, passing, 0).wait_send()

    pair().wait_recv()
    pair().wait_send()
    for d in range(2):
        pl.when(has[d])(lambda: side(d, 0, direct, 0).wait_send())

    @pl.when(takes_handed)
    def _():
        near_copy(handed, mine, passing, 0).wait_send()
        passed(0, tiles).wait_send()


def gathered(p_tiles, rows):
    tile = p_tiles.shape[-1]
    own = p_tiles.reshape(-1, tile, tile)
    tiles = own.shape[0]
    passing = tiles * 7 // 32 * 2
    dma = pltpu.SemaphoreType.DMA
    return pl.pallas_call(
        functools.partial(gather_kernel, rows, passing),
        out_shape=jax.ShapeDtypeStruct((5,) + own.shape, own.dtype),
        in_specs=[pl.BlockSpec(memory_space=pltpu.HBM)],
        out_specs=pl.BlockSpec(memory_space=pltpu.VMEM),
        scratch_shapes=[
            dma((2,)),
            dma((2, tiles - passing)),
            dma((2,)),
            dma((2, passing)),
            dma((2,)),
            dma((2,)),
            dma,
        ],
        compiler_params=pltpu.CompilerParams(
            collective_id=1, has_side_effects=True, vmem_limit_bytes=16 * 1024 * 1024
        ),
    )(own)


def body(a_tiles, a_cols, p_tiles, p_cols, c_cols):
    fine_rows = a_tiles.shape[0]
    coarse_rows = fine_rows // RATIO
    tile = a_tiles.shape[-1]
    kc = c_cols.shape[1]
    chunks = lax.axis_size("grp")
    position = lax.axis_index("row")
    band = gathered(p_tiles, lax.axis_size("row"))
    band = band.reshape((5 * fine_rows,) + p_tiles.shape[1:])
    halves, left, slot_of, links = local_products(a_tiles, a_cols, band, p_cols, position)
    out = exchange(halves, left, slot_of, links, p_cols, c_cols, lax.axis_size("row"), chunks)
    return out.reshape(coarse_rows, kc // chunks, tile, tile)


def solution(mesh):
    return jax.shard_map(
        body,
        mesh=mesh,
        in_specs=(
            P("row", "grp", None, None, None),
            P("row", "grp", None),
            P("row", None, None, None),
            P(),
            P(),
        ),
        out_specs=P("row", "grp", None, None),
        check_vma=False,
    )
```

```python
import functools

import jax
import jax.numpy as jnp
from jax import lax
from jax.experimental import pallas as pl
from jax.experimental.pallas import tpu as pltpu
from jax.sharding import PartitionSpec as P

RATIO = 2
REACH = 2


LEVELS = 32767.0


def encoded(value):
    most = jnp.maximum(jnp.max(jnp.abs(value), axis=0, keepdims=True), 2e-34)
    code = jnp.round(value * (LEVELS / most)).astype(jnp.int32).astype(jnp.int16)
    return code, most * (1.0 / LEVELS)


def decoded(code, scale):
    return code.astype(jnp.int32).astype(jnp.float32) * scale


def product_kernel(
    sizes,
    where,
    a_cols,
    p_cols,
    a_ref,
    band_ref,
    halves,
    left_ref,
    slot_of,
    links,
    sums,
):
    fine_rows, slots, kp, tile = sizes
    coarse_rows = fine_rows // RATIO
    window = (2 * (REACH + 2) + 1) * coarse_rows
    entries = slots * kp
    empty = fine_rows * entries
    position = where[0]
    first_row = position * fine_rows
    band_start = first_row - REACH * fine_rows
    window_start = (position - REACH - 2) * coarse_rows
    base_coarse = (position - 1) * coarse_rows
    halves[empty] = jnp.zeros((2 * tile, tile), jnp.bfloat16)
    sums[entries] = jnp.zeros((tile, tile), jnp.float32)

    for c in range(3 * coarse_rows):
        links[fine_rows * kp + c] = 0

    @pl.loop(0, fine_rows, unroll=4)
    def _(i):
        for w in range(window):
            slot_of[i * window + w] = empty
        for q in range(kp):
            left_ref[i * kp + q] = band_ref[(REACH * fine_rows + i) * kp + q].T
            e = i * kp + q
            c = fine_rows * kp + p_cols[q, first_row + i] - base_coarse
            links[e] = links[c]
            links[c] = e + 1
        for s in range(slots):
            j = a_cols[s, 0, i]
            local = (j - band_start) * kp
            right = jnp.concatenate([band_ref[local + p] for p in range(kp)], axis=1)
            prod = jnp.dot(a_ref[i * slots + s], right, preferred_element_type=jnp.float32)
            for p in range(kp):
                at = i * window + p_cols[p, j] - window_start
                before = jnp.minimum(slot_of[at] - i * entries, entries)
                now = s * kp + p
                slot_of[at] = i * entries + now
                value = sums[before] + prod[:, p * tile : (p + 1) * tile]
                sums[now] = value
                high = value.astype(jnp.bfloat16)
                halves[i * entries + now, :tile] = high
                halves[i * entries + now, tile:] = (
                    value - high.astype(jnp.float32)
                ).astype(jnp.bfloat16)


def local_products(a_tiles, a_cols, band, p_cols, position):
    fine_rows, _, slots, tile, _ = a_tiles.shape
    kp = band.shape[1]
    coarse_rows = fine_rows // RATIO
    window = (2 * (REACH + 2) + 1) * coarse_rows
    entries = slots * kp
    smem = pl.BlockSpec(memory_space=pltpu.SMEM)
    vmem = pl.BlockSpec(memory_space=pltpu.VMEM)
    return pl.pallas_call(
        functools.partial(product_kernel, (fine_rows, slots, kp, tile)),
        out_shape=[
            jax.ShapeDtypeStruct((fine_rows * entries + 1, 2 * tile, tile), jnp.bfloat16),
            jax.ShapeDtypeStruct((fine_rows * kp, tile, tile), jnp.bfloat16),
            jax.ShapeDtypeStruct((fine_rows * window,), jnp.int32),
            jax.ShapeDtypeStruct((fine_rows * kp + 3 * coarse_rows,), jnp.int32),
        ],
        in_specs=[smem] * 3 + [vmem] * 2,
        out_specs=[vmem] * 2 + [smem] * 2,
        scratch_shapes=[pltpu.VMEM((entries + 1, tile, tile), jnp.float32)],
        compiler_params=pltpu.CompilerParams(vmem_limit_bytes=28 * 1024 * 1024),
    )(
        position.reshape(1),
        a_cols.T,
        p_cols.T,
        a_tiles.reshape(-1, tile, tile),
        band.reshape(-1, tile, tile),
    )


def exchange_kernel(
    sizes,
    p_cols,
    c_cols,
    slot_of,
    links,
    halves,
    left_ref,
    out,
    runs,
    center,
    codes,
    scales,
    got_codes,
    got_scales,
    sent_codes,
    sent_scales,
    peer_codes,
    peer_scales,
    hop_codes,
    hop_scales,
    side_sems,
    side_scale_sems,
    peer_sems,
    peer_scale_sems,
    hop_sems,
    hop_scale_sems,
):
    fine_rows, kp, kc, tile, rows, groups = sizes
    r = lax.axis_index("row")
    g = lax.axis_index("grp")
    coarse_rows = fine_rows // RATIO
    window = (2 * (REACH + 2) + 1) * coarse_rows
    window_start = (r - REACH - 2) * coarse_rows
    first_row = r * fine_rows
    share = kc // groups
    half = share // 2
    members = half * coarse_rows
    pieces = min(fine_rows, members) // 2
    size = members // pieces
    pace = fine_rows // pieces
    bent = half // 2
    turned = bent * coarse_rows // size
    odd = lax.rem(r, 2)
    toward = 2 * odd - 1
    outer, inner = r + toward, r - toward
    has_outer = (outer >= 0) & (outer < rows)
    g_odd = lax.rem(g, 2)
    g_high = lax.rem(g // 2, 2)
    near = (g + 1 - 2 * g_odd, g + 2 - 4 * g_high)
    far = near[0] + 2 - 4 * g_high
    wanted = ((far, far), (near[0], near[1]), (near[1], near[0]), (g, g))
    steps = len(wanted)
    barrier = pltpu.get_barrier_semaphore()
    mesh_type = pl.DeviceIdType.MESH

    def signal(to):
        pl.semaphore_signal(barrier, inc=1, device_id=to, device_id_type=mesh_type)

    signal({"row": inner})
    signal({"grp": near[0]})
    signal({"grp": near[1]})
    pl.when(has_outer)(lambda: signal({"row": outer}))

    def copy(src, dst, sems, at, to):
        return pltpu.make_async_remote_copy(
            src_ref=src,
            dst_ref=dst,
            send_sem=sems.at[(0,) + at],
            recv_sem=sems.at[(1,) + at],
            device_id=to,
            device_id_type=mesh_type,
        )

    def side_scales(pos, t):
        to = {"row": inner if pos else outer}
        return (copy(scales.at[pos, t], got_scales.at[pos, t], side_scale_sems, (pos, t), to),)

    def side_piece(pos, t, part, n):
        to = {"row": inner if pos else outer}
        some = pl.ds(part * members + n * size, size)
        at = (pos, t, part, n)
        return (copy(codes.at[pos, t, some], got_codes.at[pos, t, some], side_sems, at, to),)

    def hop_copies(part):
        to = {"grp": near[part]}
        some = pl.ds(part * members, turned * size)
        return (
            copy(scales.at[0, 0, some], hop_scales.at[part], hop_scale_sems, (part,), to),
            copy(codes.at[0, 0, some], hop_codes.at[part], hop_sems, (part,), to),
        )

    def peer_piece(part, t, n):
        to = {"grp": near[part]}
        some = pl.ds(n * size, size)
        at = (part, t, n)
        return (
            copy(
                sent_scales.at[part, t, some],
                peer_scales.at[part, t, some],
                peer_scale_sems,
                at,
                to,
            ),
            copy(
                sent_codes.at[part, t, some],
                peer_codes.at[part, t, some],
                peer_sems,
                at,
                to,
            ),
        )

    def start(copies):
        for one in copies:
            one.start()

    def arrive(copies):
        for one in copies:
            one.wait_recv()

    def leave(copies):
        for one in copies:
            one.wait_send()

    runs[0] = jnp.zeros(runs.shape[1:], jnp.float32)

    @pl.when(jnp.logical_not(has_outer))
    def _():
        got_scales[0] = jnp.zeros(got_scales.shape[1:], jnp.float32)

        @pl.loop(0, 2 * members)
        def _(m):
            for t in range(steps):
                got_codes[0, t, m] = jnp.zeros((tile, tile), jnp.int16)

    def compute(t, i):
        for q in range(kp):
            e = i * kp + q
            c = p_cols[q, first_row + i]
            own = left_ref[e]
            left = jnp.concatenate([own, own], axis=1)
            parts = []
            for n in range(share):
                k = wanted[t][n // half] * share + n
                w = jnp.clip(c_cols[k, c] - window_start, 0, window - 1)
                parts.append(halves[slot_of[i * window + w]])
            prod = jnp.dot(
                left, jnp.concatenate(parts, axis=1), preferred_element_type=jnp.float32
            )
            before = links[e]
            for n in range(share):
                runs[e + 1, n] = runs[before, n] + prod[:, n * tile : (n + 1) * tile]

    def last(block, c):
        return links[fine_rows * kp + block * coarse_rows + c]

    def encode(t, pos):
        block = 2 * (1 - odd) if pos else 2 * odd

        @pl.loop(0, coarse_rows)
        def _(c):
            at = last(block, c)
            for n in range(share):
                m = n * coarse_rows + c
                value = runs[at, n]
                if t == 2 and pos == 0 and n % half < bent:
                    at_hop = n % half * coarse_rows + c
                    value += decoded(
                        hop_codes[n // half, at_hop], hop_scales[n // half, at_hop]
                    )
                code, scale = encoded(value)
                codes[pos, t, m] = code
                scales[pos, t, m] = scale

    def keep(t):
        @pl.loop(0, coarse_rows)
        def _(c):
            at = last(1, c)
            for n in range(share):
                center[t, n * coarse_rows + c] = runs[at, n]

    def each_piece(act, pos, t):
        for n in range(0 if t or pos else turned, pieces):
            for part in range(2):
                act(side_piece(pos, t, part, n))

    def send(t):
        @pl.when(has_outer)
        def _():
            if t == 2:
                for part in range(2):
                    arrive(hop_copies(part))
            encode(t, 0)

        if t == 0:
            pl.when(has_outer)(lambda: pl.semaphore_wait(barrier, 4))
            pl.when(jnp.logical_not(has_outer))(lambda: pl.semaphore_wait(barrier, 3))

        @pl.when(has_outer)
        def _():
            start(side_scales(0, t))
            each_piece(start, 0, t)
            if t == 0:
                for part in range(2):
                    start(hop_copies(part))

        encode(t, 1)
        start(side_scales(1, t))
        each_piece(start, 1, t)
        keep(t)

    def summed(t, m, skip=0):
        value = center[t, m]
        for pos in range(skip, 2):
            value += decoded(got_codes[pos, t, m], got_scales[pos, t, m])
        return value

    def peer(n, t, m):
        return decoded(peer_codes[n, t, m], peer_scales[n, t, m])

    def open_step(t, pos):
        if pos:
            arrive(side_scales(1, t))
        else:
            pl.when(has_outer)(lambda: arrive(side_scales(0, t)))

    def come(t, part, n, skip=0):
        if not skip:
            pl.when(has_outer)(lambda: arrive(side_piece(0, t, part, n)))
        arrive(side_piece(1, t, part, n))

    def forward(t, n, skip=0):
        for part in range(2):
            to = 1 - part if t == 2 else part
            come(t, part, n, skip)
            if t == 2:
                arrive(peer_piece(part, 0, n))
            for u in range(size):
                m = n * size + u
                value = summed(t, part * members + m, skip)
                if t == 2:
                    value += peer(part, 0, m)
                code, scale = encoded(value)
                sent_codes[to, t, m] = code
                sent_scales[to, t, m] = scale
            start(peer_piece(to, t, n))

    def finish(t, n):
        for part in range(2):
            come(t, part, n)
            arrive(peer_piece(part, 1, n))
            arrive(peer_piece(1 - part, 2, n))
            for u in range(size):
                m = n * size + u
                c = lax.rem(m, coarse_rows)
                k = part * half + m // coarse_rows
                value = summed(t, part * members + m)
                out[c * share + k] = value + peer(part, 1, m) + peer(1 - part, 2, m)

    pl.loop(0, fine_rows, unroll=4)(lambda i: compute(0, i))
    send(0)
    open_step(0, 1)

    @pl.loop(0, turned)
    def _(n):
        for u in range(pace):
            compute(1, n * pace + u)
        forward(0, n, 1)

    pl.loop(turned * pace, fine_rows, unroll=4)(lambda i: compute(1, i))
    send(1)
    open_step(0, 0)
    quick = fine_rows // (pieces - turned)

    @pl.loop(turned, pieces)
    def _(n):
        forward(0, n)
        for u in range(quick):
            compute(2, (n - turned) * quick + u)

    send(2)
    open_step(1, 1)
    open_step(1, 0)

    @pl.loop(0, pieces)
    def _(n):
        forward(1, n)
        for u in range(pace):
            compute(3, n * pace + u)

    send(3)
    open_step(2, 1)
    open_step(2, 0)
    pl.loop(0, pieces)(lambda n: forward(2, n))
    open_step(3, 1)
    open_step(3, 0)
    pl.loop(0, pieces)(lambda n: finish(3, n))
    for t in range(steps):

        @pl.when(has_outer)
        def _():
            leave(side_scales(0, t))
            each_piece(leave, 0, t)
            if t == 0:
                for part in range(2):
                    leave(hop_copies(part))

        leave(side_scales(1, t))
        each_piece(leave, 1, t)
    for t in range(steps - 1):
        for part in range(2):
            for n in range(pieces):
                leave(peer_piece(part, t, n))


def exchange(halves, left, slot_of, links, p_cols, c_cols, rows, groups):
    _, tile = halves.shape[1:]
    kp = p_cols.shape[1]
    kc = c_cols.shape[1]
    fine_rows = left.shape[0] // kp
    coarse_rows = fine_rows // RATIO
    share = kc // groups
    members = share * coarse_rows
    pieces = min(fine_rows, members // 2) // 2
    steps = 4
    smem = pl.BlockSpec(memory_space=pltpu.SMEM)
    vmem = pl.BlockSpec(memory_space=pltpu.VMEM)
    dma = pltpu.SemaphoreType.DMA

    def tiles(*lead):
        return [
            pltpu.VMEM(lead + (tile, tile), jnp.int16),
            pltpu.VMEM(lead + (1, tile), jnp.float32),
        ]

    return pl.pallas_call(
        functools.partial(exchange_kernel, (fine_rows, kp, kc, tile, rows, groups)),
        out_shape=jax.ShapeDtypeStruct((members, tile, tile), jnp.float32),
        in_specs=[smem] * 4 + [vmem] * 2,
        out_specs=vmem,
        scratch_shapes=[
            pltpu.VMEM((fine_rows * kp + 1, share, tile, tile), jnp.float32),
            pltpu.VMEM((steps, members, tile, tile), jnp.float32),
            *tiles(2, steps, members),
            *tiles(2, steps, members),
            *tiles(2, steps - 1, members // 2),
            *tiles(2, steps - 1, members // 2),
            *tiles(2, share // 4 * coarse_rows),
            dma((2, 2, steps, 2, pieces)),
            dma((2, 2, steps)),
            dma((2, 2, steps - 1, pieces)),
            dma((2, 2, steps - 1, pieces)),
            dma((2, 2)),
            dma((2, 2)),
        ],
        compiler_params=pltpu.CompilerParams(
            collective_id=0, has_side_effects=True, vmem_limit_bytes=28 * 1024 * 1024
        ),
    )(p_cols.T, c_cols.T, slot_of, links, halves, left)


def gather_kernel(
    rows,
    passing,
    own,
    band,
    side_sends,
    side_comes,
    near_sends,
    near_comes,
    pair_sems,
    pass_sems,
    own_sem,
):
    r = lax.axis_index("row")
    g = lax.axis_index("grp")
    odd = lax.rem(r, 2)
    partner = r + 1 - 2 * odd
    has = (r >= 2, r < rows - 2)
    handed, kept = odd, 1 - odd
    takes_handed = jnp.where(odd == 0, r < rows - 2, r >= 2)
    takes_kept = jnp.where(odd == 0, r >= 2, r < rows - 2)
    g_odd = lax.rem(g, 2)
    g_high = lax.rem(g // 2, 2)
    near = (g + 1 - 2 * g_odd, g + 2 - 4 * g_high)
    parity = lax.rem(g_odd + g_high, 2)
    tiles = own.shape[0]
    direct = tiles - passing
    mine = parity * direct
    other = (1 - parity) * direct
    barrier = pltpu.get_barrier_semaphore()
    mesh_type = pl.DeviceIdType.MESH
    local = pltpu.make_async_copy(own, band.at[2], own_sem)
    local.start()

    def copy(src, dst, send, recv, to):
        return pltpu.make_async_remote_copy(
            src_ref=src,
            dst_ref=dst,
            send_sem=send,
            recv_sem=recv,
            device_id=to,
            device_id_type=mesh_type,
        )

    def place(n):
        return mine + n if n < passing else n

    def side(d, at, size, n):
        part = pl.ds(at, size)
        return copy(
            band.at[2, part],
            band.at[4 - 4 * d, part],
            side_sends.at[d],
            side_comes.at[d, n],
            {"row": r - 2 + 4 * d},
        )

    def near_copy(d, at, size, n):
        ref = band.at[4 - 4 * d, pl.ds(at, size)]
        to = {"grp": near[n % 2]}
        return copy(ref, ref, near_sends.at[d], near_comes.at[d, n], to)

    def pair():
        return copy(
            band.at[2],
            band.at[1 + 2 * odd],
            pair_sems.at[0],
            pair_sems.at[1],
            {"row": partner},
        )

    def passed(at, size):
        part = pl.ds(at, size)
        return copy(
            band.at[4 - 4 * odd, part],
            band.at[3 - 2 * odd, part],
            pass_sems.at[0],
            pass_sems.at[1],
            {"row": partner},
        )

    def signal(to):
        pl.semaphore_signal(barrier, inc=1, device_id=to, device_id_type=mesh_type)

    signal({"row": partner})
    signal({"grp": near[0]})
    signal({"grp": near[1]})
    for d in range(2):
        pl.when(has[d])(lambda: signal({"row": r - 2 + 4 * d}))
    local.wait()
    pl.when(has[0] & has[1])(lambda: pl.semaphore_wait(barrier, 5))
    pl.when(jnp.logical_not(has[0] & has[1]))(lambda: pl.semaphore_wait(barrier, 4))

    for d in range(2):

        @pl.when(has[d])
        def _():
            for n in range(direct):
                side(d, place(n), 1, n).start()

    pair().start()

    for n in range(direct):

        @pl.when(takes_handed)
        def _():
            side(handed, place(n), 1, n).wait_recv()
            if n < passing:
                near_copy(handed, mine + n, 1, n).start()
            passed(place(n), 1).start()

        if n < passing:

            @pl.when(takes_kept)
            def _():
                side(kept, place(n), 1, n).wait_recv()
                near_copy(kept, mine + n, 1, n).start()

    @pl.when(takes_handed)
    def _():
        for n in range(passing):
            near_copy(handed, other + n, 1, n).wait_recv()
            passed(other + n, 1).start()

    @pl.when(takes_kept)
    def _():
        for n in range(passing, direct):
            side(kept, place(n), 1, n).wait_recv()
        for n in range(passing):
            near_copy(kept, other + n, 1, n).wait_recv()
        passed(0, tiles).wait_recv()
        near_copy(kept, mine, passing, 0).wait_send()

    pair().wait_recv()
    pair().wait_send()
    for d in range(2):
        pl.when(has[d])(lambda: side(d, 0, direct, 0).wait_send())

    @pl.when(takes_handed)
    def _():
        near_copy(handed, mine, passing, 0).wait_send()
        passed(0, tiles).wait_send()


def gathered(p_tiles, rows):
    tile = p_tiles.shape[-1]
    own = p_tiles.reshape(-1, tile, tile)
    tiles = own.shape[0]
    passing = tiles * 7 // 32 * 2
    dma = pltpu.SemaphoreType.DMA
    return pl.pallas_call(
        functools.partial(gather_kernel, rows, passing),
        out_shape=jax.ShapeDtypeStruct((5,) + own.shape, own.dtype),
        in_specs=[pl.BlockSpec(memory_space=pltpu.HBM)],
        out_specs=pl.BlockSpec(memory_space=pltpu.VMEM),
        scratch_shapes=[
            dma((2,)),
            dma((2, tiles - passing)),
            dma((2,)),
            dma((2, passing)),
            dma((2,)),
            dma((2,)),
            dma,
        ],
        compiler_params=pltpu.CompilerParams(
            collective_id=1, has_side_effects=True, vmem_limit_bytes=16 * 1024 * 1024
        ),
    )(own)


def body(a_tiles, a_cols, p_tiles, p_cols, c_cols):
    fine_rows = a_tiles.shape[0]
    coarse_rows = fine_rows // RATIO
    tile = a_tiles.shape[-1]
    kc = c_cols.shape[1]
    chunks = lax.axis_size("grp")
    position = lax.axis_index("row")
    band = gathered(p_tiles, lax.axis_size("row"))
    band = band.reshape((5 * fine_rows,) + p_tiles.shape[1:])
    halves, left, slot_of, links = local_products(a_tiles, a_cols, band, p_cols, position)
    out = exchange(halves, left, slot_of, links, p_cols, c_cols, lax.axis_size("row"), chunks)
    return out.reshape(coarse_rows, kc // chunks, tile, tile)


def solution(mesh):
    return jax.shard_map(
        body,
        mesh=mesh,
        in_specs=(
            P("row", "grp", None, None, None),
            P("row", "grp", None),
            P("row", None, None, None),
            P(),
            P(),
        ),
        out_specs=P("row", "grp", None, None),
        check_vma=False,
    )
```
